512 devices in a mesh: groups: 2 (over y), ctx: 32 (over z), ep: 4 (over x), tp: 2 (over core).
Axes of the slice: x: 4, y: 2, z: 32, core: 2. Of those that a mesh axis runs over, the one named last changes fastest.
The devices are a block of a 4x8x32 slice.
Arguments:
- queries: bfloat16 [8, 4096, 5120], P(('groups', 'ep'), 'ctx', 'tp'), parts along dimension 0, may hold values from -128 to 128
- keys: bfloat16 [8, 4096, 1024], P(('groups', 'ep'), 'ctx', 'tp'), parts along dimension 0, may hold values from -6 to 6
- values: bfloat16 [8, 4096, 1024], P(('groups', 'ep'), 'ctx', 'tp'), parts along dimension 0, may hold values from -6 to 6
- expert_ids: int32 [8, 4096, 1], P(('groups', 'ep'), 'ctx'), parts along dimension 0, may hold values from 0 to 127, as said below
- router: bfloat16 [5120, 4], P('tp', 'ep'), may hold values from -0.3125 to 0.3125
- w_gate: bfloat16 [4, 5120, 4096], P('ep', 'tp', 'ctx'), may hold values from -0.3125 to 0.3125
- w_up: bfloat16 [4, 5120, 4096], P('ep', 'tp', 'ctx'), may hold values from -0.3125 to 0.3125
- w_down: bfloat16 [4, 4096, 5120], P('ep', 'ctx', 'tp'), may hold values from -0.09375 to 0.09375
Outputs:
- layer_out: bfloat16 [8, 4096, 5120], P(('groups', 'ep'), 'ctx', 'tp'), parts along dimension 0
The draws below stay inside these ranges and needn't reach their ends.
There are 2 independent parts, one for each index of `groups`. The reference program is written for one: setup_inputs(seed, part) draws one part's arguments, and reference() takes and returns one part's arrays. A program takes and returns all parts, laid end to end along the dimension named above; an argument that names none is the same for every part. Nothing has to cross between parts.
Inputs may be any that keep to these rules, and one draw needn't show every extreme that they name: `expert_ids`: among the positions of one device, each expert below 4 is named at most 2 times; in every draw one of them is named exactly 2 times on every device.
All inputs are finite; a program needn't handle non-finite values.
Results may differ from the reference program's by a relative error of at most 0.023.
Values may be sent and summed in bfloat16 or wider, within the bound.
No kernel may reach another device: no remote copies, remote signals or barrier semaphores. Data moves between devices by JAX's collectives and lax.ppermute only.
A program may use at most 64 MiB of HBM per device.

```python
import math
import jax
import jax.numpy as jnp
from jax import lax

HEAD_WIDTH = 128
QUERY_HEADS = 40
KEY_VALUE_HEADS = 8
D = 5120
EXPERTS = 128
FE = 4096
SEQ_DEV = 128
PROMPT_LENGTH = 4096
PROMPT_BATCH = 4
EXP_WIN = 4
CAP = 2


def shared_keys(key):
    return jax.random.truncated_normal(jax.random.fold_in(key, 11), -6.0, 6.0, (PROMPT_BATCH, PROMPT_LENGTH, KEY_VALUE_HEADS, HEAD_WIDTH), jnp.float32)


def draw_keys(key, part):
    unprojected_keys = shared_keys(key)
    return unprojected_keys.reshape(PROMPT_BATCH, PROMPT_LENGTH, KEY_VALUE_HEADS * HEAD_WIDTH).astype(jnp.bfloat16)


def draw_queries(key, part):
    base = 2.5 * jax.random.truncated_normal(jax.random.fold_in(key, 23), -6.0, 6.0, (PROMPT_BATCH, PROMPT_LENGTH, QUERY_HEADS, HEAD_WIDTH), jnp.float32)
    return base.reshape(PROMPT_BATCH, PROMPT_LENGTH, QUERY_HEADS * HEAD_WIDTH).astype(jnp.bfloat16)


def shuffled(sub_key):
    return jax.random.permutation(sub_key, SEQ_DEV)


def draw_expert_ids(key, part):
    blocks = PROMPT_BATCH * (PROMPT_LENGTH // SEQ_DEV)
    count_key = jax.random.fold_in(key, 41)
    full_key = jax.random.fold_in(key, 43)
    outside_key = jax.random.fold_in(key, 47)
    order_key = jax.random.fold_in(key, 53)
    counts = jax.random.randint(count_key, (blocks, EXP_WIN), 0, CAP + 1, dtype=jnp.int32)
    full_expert = jax.random.randint(full_key, (), 0, EXP_WIN, dtype=jnp.int32)
    counts = jnp.where(jnp.arange(EXP_WIN, dtype=jnp.int32)[None, :] == full_expert, CAP, counts)
    count_ends = jnp.cumsum(counts, axis=1)
    rank_index = jnp.arange(SEQ_DEV, dtype=jnp.int32)
    expert_rank = jnp.sum((count_ends[:, None, :] <= rank_index[None, :, None]).astype(jnp.int32), axis=2)
    outside = jax.random.randint(outside_key, (blocks, SEQ_DEV), EXP_WIN, EXPERTS, dtype=jnp.int32)
    named = jnp.where(expert_rank < EXP_WIN, expert_rank, outside)
    shuffles = jax.vmap(shuffled)(jax.random.split(order_key, blocks))
    inverse = jnp.argsort(shuffles, axis=1)
    placed = jnp.take_along_axis(named, inverse, axis=1)
    return placed.reshape(PROMPT_BATCH, PROMPT_LENGTH, 1).astype(jnp.int32)


def block_levels(stream_key, shape, cuts, smallest, largest):
    gain = 1.0
    for dim, parts in cuts:
        steps = jax.random.uniform(jax.random.fold_in(jax.random.fold_in(stream_key, 6), dim), (parts,), jnp.float32, smallest / len(cuts), largest / len(cuts))
        gain = gain * jnp.repeat(jnp.exp(steps), shape[dim] // parts).reshape((-1,) + (1,) * (len(shape) - 1 - dim))
    return gain


def normal_values(stream_key, dims, deviation, most, cuts=(), kind=jnp.bfloat16):
    drawn = deviation * jax.random.normal(stream_key, dims, jnp.float32)
    if cuts:
        drawn = drawn * block_levels(stream_key, dims, cuts, -0.22, 0.18)
    return jnp.clip(drawn, -most, most).astype(kind)


def setup_inputs(seed: int = 0, part: int = 0) -> dict:
    arg_keys = jax.random.split(jax.random.key(seed), 9)
    own_keys = jax.random.split(jax.random.fold_in(arg_keys[8], part), 9)
    return {
        "queries": draw_queries(jax.random.fold_in(jax.random.fold_in(arg_keys[8], part), 71), part),
        "keys": draw_keys(jax.random.fold_in(jax.random.fold_in(arg_keys[8], part), 71), part),
        "values": normal_values(own_keys[2], (PROMPT_BATCH, PROMPT_LENGTH, KEY_VALUE_HEADS * HEAD_WIDTH), 1.0, 6.0, ((0, 4), (1, 32), (2, 2))),
        "expert_ids": draw_expert_ids(jax.random.fold_in(jax.random.fold_in(arg_keys[8], part), 71), part),
        "router": normal_values(arg_keys[4], (D, EXP_WIN), (D // 16) ** -0.5, 0.3125, ((0, 2), (1, 4))),
        "w_gate": normal_values(arg_keys[5], (EXP_WIN, D, FE), (D // 16) ** -0.5, 0.3125, ((0, 4), (1, 2), (2, 32))),
        "w_up": normal_values(arg_keys[6], (EXP_WIN, D, FE), (D // 16) ** -0.5, 0.3125, ((0, 4), (1, 2), (2, 32))),
        "w_down": normal_values(arg_keys[7], (EXP_WIN, FE, D), FE ** -0.5, 0.09375, ((0, 4), (1, 32), (2, 2))),
    }


def attend_sequence(query_sequence, key_sequence, value_sequence):
    group_width = QUERY_HEADS // KEY_VALUE_HEADS
    rows_per_block = math.gcd(PROMPT_LENGTH, 256)
    query_block_list = query_sequence.reshape(PROMPT_LENGTH // rows_per_block, rows_per_block, KEY_VALUE_HEADS, group_width, HEAD_WIDTH)
    complete_keys = key_sequence.reshape(PROMPT_LENGTH, KEY_VALUE_HEADS, HEAD_WIDTH).astype(jnp.float32)
    complete_values = value_sequence.reshape(PROMPT_LENGTH, KEY_VALUE_HEADS, HEAD_WIDTH).astype(jnp.float32)
    key_pos = jnp.arange(PROMPT_LENGTH, dtype=jnp.int32)

    def one_block(inputs):
        query_block, begin_row = inputs
        scores = jnp.einsum("rgqd,kgd->gqrk", query_block.astype(jnp.float32), complete_keys) * (HEAD_WIDTH ** -0.5)
        query_pos = begin_row + jnp.arange(rows_per_block, dtype=jnp.int32)
        visible = query_pos[:, None] >= key_pos[None, :]
        scores = jnp.where(visible, scores, -1e30)
        row_max = jnp.max(scores, axis=3, keepdims=True)
        weights = jnp.where(visible, jnp.exp(scores - row_max), 0.0)
        totals = jnp.sum(weights, axis=3)
        rounded = lax.optimization_barrier(weights.astype(jnp.bfloat16)).astype(jnp.float32)
        weighted = jnp.einsum("gqrk,kgd->rgqd", rounded, complete_values)
        normed = weighted / jnp.transpose(totals, (2, 0, 1))[..., None]
        return normed.astype(jnp.bfloat16).reshape(rows_per_block, D)

    starts = jnp.arange(PROMPT_LENGTH // rows_per_block, dtype=jnp.int32) * rows_per_block
    return lax.map(one_block, (query_block_list, starts)).reshape(PROMPT_LENGTH, D)


def reference(queries, keys, values, expert_ids, router, w_gate, w_up, w_down):
    attended = jnp.stack([attend_sequence(queries[prompt], keys[prompt], values[prompt]) for prompt in range(PROMPT_BATCH)])
    token_count = PROMPT_BATCH * PROMPT_LENGTH
    flat_tokens = attended.reshape(token_count, D)
    chosen = expert_ids.reshape(token_count).astype(jnp.int32)
    sort_order = jnp.argsort(chosen, stable=True).astype(jnp.int32)
    counts = jnp.sum((chosen[:, None] == jnp.arange(EXP_WIN, dtype=jnp.int32)[None, :]).astype(jnp.int32), axis=0)
    offsets = (jnp.cumsum(counts) - counts).astype(jnp.int32)
    most_rows = CAP * PROMPT_BATCH * (PROMPT_LENGTH // SEQ_DEV)
    padded_order = jnp.concatenate([sort_order, jnp.zeros((most_rows,), jnp.int32)])

    def expert_step(routed, inputs):
        expert, gate_w, up_w, down_w, router_col = inputs
        picked = lax.dynamic_slice_in_dim(padded_order, offsets[expert], most_rows)
        live_rows = jnp.arange(most_rows, dtype=jnp.int32) < counts[expert]
        members = flat_tokens[picked]
        gate_part = jnp.dot(members, gate_w, preferred_element_type=jnp.float32)
        up_part = jnp.dot(members, up_w, preferred_element_type=jnp.float32)
        router_score = jnp.dot(members, router_col[:, None], preferred_element_type=jnp.float32)
        weight = jax.nn.sigmoid(router_score)
        hidden = (jax.nn.silu(weight * gate_part) * (weight * up_part)).astype(jnp.bfloat16)
        output = jnp.dot(hidden, down_w, preferred_element_type=jnp.float32).astype(jnp.bfloat16)
        output = lax.optimization_barrier(output).astype(jnp.float32)
        output = jnp.where(live_rows[:, None], output, 0.0)
        return routed.at[picked].add(output), None

    routed, _ = lax.scan(expert_step, jnp.zeros((token_count, D), jnp.float32),
                         (jnp.arange(EXP_WIN, dtype=jnp.int32), w_gate, w_up, w_down, router.T))
    layer_out = (flat_tokens.astype(jnp.float32) + routed).astype(jnp.bfloat16)
    return layer_out.reshape(PROMPT_BATCH, PROMPT_LENGTH, D)
```

```python
import functools

import jax
import jax.numpy as jnp
from jax import lax
from jax.experimental import pallas as pl
from jax.experimental.pallas import tpu as pltpu
from jax.sharding import Mesh, PartitionSpec as P

HEAD_WIDTH = 128
CAP = 2
NEAR = 8
CTX = ("far", "near")
MASKED = -1e30
EXP2_SCALE = HEAD_WIDTH ** (-0.5) * 1.4426950408889634
STEPS_PER_CALL = 2
INTERPRET = False


def heads_to_rows(block):
    heads = block.shape[1] // HEAD_WIDTH
    return jnp.concatenate(
        [block[:, j * HEAD_WIDTH : (j + 1) * HEAD_WIDTH] for j in range(heads)], axis=0
    )


def attend_kernel(seen_ref, q_ref, *refs, block_count, own_first, first, last):
    k_refs = refs[:block_count]
    v_refs = refs[block_count : 2 * block_count]
    rest = refs[2 * block_count :]
    row_count = q_ref.shape[0]
    q = heads_to_rows(q_ref[...])
    rows = q.shape[0]
    keys = jnp.concatenate([r[...] for r in k_refs], axis=0)
    values = jnp.concatenate([r[...] for r in v_refs], axis=0)
    scores = lax.dot_general(
        keys, q, (((1,), (1,)), ((), ())), preferred_element_type=jnp.float32
    )
    width = k_refs[0].shape[0]

    def folded(piece, reduce):
        return reduce(piece.reshape(width // 8, 8, rows), axis=0)

    pieces, visible = [], []
    top = None
    for b in range(block_count):
        piece = scores[b * width : (b + 1) * width]
        if own_first and b == 0:
            key_place = lax.broadcasted_iota(jnp.int32, piece.shape, 0)
            query_place = lax.broadcasted_iota(jnp.int32, piece.shape, 1) % row_count
            piece = jnp.where(query_place >= key_place, piece, MASKED)
            block_top = folded(piece, jnp.max)
            visible.append(None)
        else:
            visible.append(seen_ref[b] > 0)
            block_top = jnp.where(visible[b], folded(piece, jnp.max), MASKED)
        pieces.append(piece)
        top = block_top if top is None else jnp.maximum(top, block_top)
    new_max = jnp.max(top, axis=0, keepdims=True) * EXP2_SCALE
    if not first:
        acc_ref, max_ref, total_ref = rest[:3]
        rest = rest[3:]
        old_max = max_ref[0, 0:1, :]
        new_max = jnp.maximum(new_max, old_max)
        factor = jnp.exp2(old_max - new_max)
    total = None
    weights = []
    for piece, seen in zip(pieces, visible):
        below = new_max if seen is None else jnp.where(seen, new_max, -MASKED)
        weight = jnp.exp2(piece * EXP2_SCALE - below)
        weights.append(weight.astype(jnp.bfloat16))
        part = folded(weight, jnp.sum)
        total = part if total is None else total + part
    rounded = jnp.concatenate(weights, axis=0)
    acc = lax.dot_general(
        values, rounded, (((0,), (0,)), ((), ())), preferred_element_type=jnp.float32
    )
    if not first:
        total = total + total_ref[0] * factor
        acc = acc + acc_ref[0] * factor
    if last:
        out = acc / jnp.sum(total, axis=0, keepdims=True)
        out_ref = rest[0]
        for j in range(rows // row_count):
            out_ref[:, j * HEAD_WIDTH : (j + 1) * HEAD_WIDTH] = out[
                :, j * row_count : (j + 1) * row_count
            ].T.astype(jnp.bfloat16)
    else:
        acc_out, max_out, total_out = rest
        acc_out[0] = acc
        max_out[0] = jnp.broadcast_to(new_max, total.shape)
        total_out[0] = total


def attend(seen, queries, keys, values, state, own_first, last):
    row_count, features = queries.shape
    block_count = len(keys)
    kv_heads = keys[0].shape[1] // HEAD_WIDTH
    group_features = features // kv_heads
    rows = row_count * group_features // HEAD_WIDTH
    width = keys[0].shape[0]
    first = state is None
    state_rows = (HEAD_WIDTH, 8, 8)
    state_specs = [pl.BlockSpec((1, n, rows), lambda g: (g, 0, 0)) for n in state_rows]
    kv_spec = pl.BlockSpec((width, HEAD_WIDTH), lambda g: (0, g))
    q_spec = pl.BlockSpec((row_count, group_features), lambda g: (0, g))
    in_specs = [pl.BlockSpec(memory_space=pltpu.SMEM), q_spec] + [kv_spec] * (2 * block_count)
    operands = [seen, queries, *keys, *values]
    if not first:
        in_specs += state_specs
        operands += list(state)
    if last:
        out_specs = q_spec
        out_shape = jax.ShapeDtypeStruct((row_count, features), jnp.bfloat16)
    else:
        out_specs = state_specs
        out_shape = [jax.ShapeDtypeStruct((kv_heads, n, rows), jnp.float32) for n in state_rows]
    pairs = rows * kv_heads * width * block_count
    return pl.pallas_call(
        functools.partial(
            attend_kernel,
            block_count=block_count,
            own_first=own_first,
            first=first,
            last=last,
        ),
        grid=(kv_heads,),
        in_specs=in_specs,
        out_specs=out_specs,
        out_shape=out_shape,
        compiler_params=pltpu.CompilerParams(vmem_limit_bytes=24 * 1024 * 1024),
        cost_estimate=pl.CostEstimate(
            flops=pairs * HEAD_WIDTH * 4, transcendentals=pairs, bytes_accessed=pairs
        ),
        name="attend",
        interpret=INTERPRET,
    )(*operands)


def expert_in_kernel(*refs, piece_count):
    pieces = refs[:piece_count]
    gate_ref, up_ref, router_ref, own_ref, sent_ref = refs[piece_count:]
    members = jnp.concatenate([r[...] for r in pieces], axis=0)
    hidden_width = gate_ref.shape[1]
    for k, w_ref in enumerate((gate_ref, up_ref, router_ref)):
        part = jnp.dot(members, w_ref[...], preferred_element_type=jnp.float32)
        own_ref[:, k * hidden_width : (k + 1) * hidden_width] = part
        sent_ref[:, k * hidden_width : (k + 1) * hidden_width] = part.astype(jnp.bfloat16)


def expert_out_kernel(own_ref, other_ref, down_ref, out_ref):
    both = own_ref[...] + other_ref[...].astype(jnp.float32)
    hidden_width = down_ref.shape[0]
    gate = both[:, :hidden_width]
    up = both[:, hidden_width : 2 * hidden_width]
    score = both[:, 2 * hidden_width :]
    weight = 1.0 / (1.0 + jnp.exp(-score))
    gated = weight * gate
    hidden = (gated / (1.0 + jnp.exp(-gated)) * (weight * up)).astype(jnp.bfloat16)
    out_ref[...] = jnp.dot(hidden, down_ref[...], preferred_element_type=jnp.float32).astype(
        jnp.bfloat16
    )


def summed(*parts):
    total = parts[0].astype(jnp.float32)
    for part in parts[1:]:
        total = total + part.astype(jnp.float32)
    return total.astype(jnp.bfloat16)


def shards(queries, keys, values, expert_ids, router, w_gate, w_up, w_down):
    row_count, features = queries.shape[1:]
    ep_count = lax.axis_size("ep")
    far_count = lax.axis_size("far")
    near_count = lax.axis_size("near")
    ctx_count = far_count * near_count
    place = lax.axis_index(CTX)

    def shift(value, step):
        return lax.ppermute(
            value, CTX, [(i, (i + step) % ctx_count) for i in range(ctx_count)]
        )

    chosen = expert_ids[0, :, 0]
    choose = (chosen[:, None] == jnp.arange(ep_count, dtype=jnp.int32)[None, :]).astype(jnp.int32)
    earlier = jnp.cumsum(choose, axis=0) - choose
    slot_index = jnp.sum(earlier * choose, axis=1)
    target = chosen * CAP + slot_index
    spread = (target[None, :] == jnp.arange(ep_count * CAP, dtype=jnp.int32)[:, None]).astype(
        jnp.bfloat16
    )
    hidden_width = w_gate.shape[2]
    router_wide = jnp.broadcast_to(router, (features, hidden_width))

    q = queries[0]
    ahead_k = back_k = keys[0]
    ahead_v = back_v = values[0]
    waiting_k, waiting_v = [ahead_k], [ahead_v]
    seen = [jnp.int32(1)]
    state = None
    own_first = True
    steps = ctx_count // 2
    for step in range(1, steps + 1):
        ahead_k = shift(ahead_k, 1)
        waiting_k.append(ahead_k)
        seen.append((place >= step).astype(jnp.int32))
        if step < ctx_count - step:
            back_k = shift(back_k, -1)
            waiting_k.append(back_k)
            seen.append((place + step >= ctx_count).astype(jnp.int32))
        if state is not None and step % STEPS_PER_CALL == 0:
            ahead_v, *state = lax.optimization_barrier((ahead_v, *state))
        ahead_v = shift(ahead_v, 1)
        waiting_v.append(ahead_v)
        if step < ctx_count - step:
            back_v = shift(back_v, -1)
            waiting_v.append(back_v)
        last = step == steps
        if step % STEPS_PER_CALL == 0 or last:
            state = attend(jnp.stack(seen), q, waiting_k, waiting_v, state, own_first, last)
            waiting_k, waiting_v, seen = [], [], []
            own_first = False
    attended = state

    outgoing = jnp.dot(spread, attended, preferred_element_type=jnp.float32).astype(jnp.bfloat16)
    exchange = ("far", "ep")
    to_all = jnp.broadcast_to(
        outgoing.reshape(1, ep_count, CAP, features), (far_count, ep_count, CAP, features)
    ).reshape(far_count * ep_count, CAP, features)
    arrived = lax.all_to_all(to_all, exchange, 0, 0, tiled=True)
    own_set = arrived.reshape(far_count * ep_count * CAP, features)

    ahead_count = near_count // 2
    back_count = near_count - 1 - ahead_count
    pieces = [own_set]
    ahead = back = own_set
    ahead_pieces, back_pieces = [], []
    for step in range(1, ahead_count + 1):
        ahead = shift(ahead, 1)
        ahead_pieces.append(ahead)
        if step <= back_count:
            back = shift(back, -1)
            back_pieces.append(back)
    pieces = [own_set] + ahead_pieces + back_pieces
    set_rows = own_set.shape[0]
    member_rows = set_rows * near_count

    own_part, sent_part = pl.pallas_call(
        functools.partial(expert_in_kernel, piece_count=near_count),
        out_shape=[
            jax.ShapeDtypeStruct((member_rows, 3 * hidden_width), jnp.float32),
            jax.ShapeDtypeStruct((member_rows, 3 * hidden_width), jnp.bfloat16),
        ],
        compiler_params=pltpu.CompilerParams(vmem_limit_bytes=24 * 1024 * 1024),
        name="expert_in",
        interpret=INTERPRET,
    )(*pieces, w_gate[0], w_up[0], router_wide)
    other_part = lax.ppermute(sent_part, "tp", [(0, 1), (1, 0)])
    partial_out = pl.pallas_call(
        expert_out_kernel,
        out_shape=jax.ShapeDtypeStruct((member_rows, features), jnp.bfloat16),
        compiler_params=pltpu.CompilerParams(vmem_limit_bytes=24 * 1024 * 1024),
        name="expert_out",
        interpret=INTERPRET,
    )(own_part, other_part, w_down[0])
    parts = [partial_out[k * set_rows : (k + 1) * set_rows] for k in range(near_count)]
    own_out = parts[0]
    ahead_out = parts[1 : 1 + ahead_count]
    back_out = parts[1 + ahead_count :]

    ahead_sum, back_sum = None, None
    for step in range(ahead_count, 0, -1):
        mine = ahead_out[step - 1]
        ahead_sum = shift(mine if ahead_sum is None else summed(mine, ahead_sum), -1)
        if step <= back_count:
            mine = back_out[step - 1]
            back_sum = shift(mine if back_sum is None else summed(mine, back_sum), 1)
    set_sum = summed(own_out, ahead_sum, back_sum)
    returned = lax.all_to_all(
        set_sum.reshape(far_count * ep_count, CAP, features), exchange, 0, 0, tiled=True
    )
    expert_rows = jnp.sum(
        returned.reshape(far_count, ep_count * CAP, features).astype(jnp.float32), axis=0
    ).astype(jnp.bfloat16)
    routed = lax.dot_general(
        spread, expert_rows, (((0,), (0,)), ((), ())), preferred_element_type=jnp.float32
    )
    layer_out = (attended.astype(jnp.float32) + routed).astype(jnp.bfloat16)
    return layer_out[None]


def solution(mesh):
    shape = dict(zip(mesh.axis_names, mesh.devices.shape))
    near = NEAR if shape["ctx"] % NEAR == 0 else shape["ctx"]
    names, sizes = [], []
    for name in mesh.axis_names:
        if name == "ctx":
            names += ["far", "near"]
            sizes += [shape[name] // near, near]
        else:
            names.append(name)
            sizes.append(shape[name])
    split = Mesh(mesh.devices.reshape(sizes), tuple(names))
    placed = (
        P(("groups", "ep"), CTX, "tp"),
        P(("groups", "ep"), CTX, "tp"),
        P(("groups", "ep"), CTX, "tp"),
        P(("groups", "ep"), CTX, None),
        P("tp", "ep"),
        P("ep", "tp", CTX),
        P("ep", "tp", CTX),
        P("ep", CTX, "tp"),
    )
    return jax.shard_map(
        shards,
        mesh=split,
        in_specs=placed,
        out_specs=P(("groups", "ep"), CTX, "tp"),
        check_vma=False,
    )
```

```python
import functools

import jax
import jax.numpy as jnp
from jax import lax
from jax.experimental import pallas as pl
from jax.experimental.pallas import tpu as pltpu
from jax.sharding import Mesh, PartitionSpec as P

HEAD_WIDTH = 128
CAP = 2
NEAR = 8
CTX = ("far", "near")
MASKED = -1e30
EXP2_SCALE = HEAD_WIDTH ** (-0.5) * 1.4426950408889634
OWN_CHUNK = 1024
INTERPRET = False


def heads_to_rows(block):
    heads = block.shape[1] // HEAD_WIDTH
    return jnp.concatenate(
        [block[:, j * HEAD_WIDTH : (j + 1) * HEAD_WIDTH] for j in range(heads)], axis=0
    )


def attend_kernel(
    span_ref, place_ref, q_ref, k_ref, v_ref, out_ref, acc_ref, max_ref, total_ref, *, chunk
):
    row_count = q_ref.shape[0]
    q = heads_to_rows(q_ref[...])
    rows = q.shape[0]
    acc_ref[...] = jnp.zeros(acc_ref.shape, jnp.float32)
    max_ref[...] = jnp.full(max_ref.shape, MASKED, jnp.float32)
    total_ref[...] = jnp.zeros(total_ref.shape, jnp.float32)

    def folded(piece, reduce):
        return reduce(piece.reshape(chunk // 8, 8, rows), axis=0)

    def absorb(index, masked):
        begin = pl.multiple_of(index * chunk, chunk)
        scores = lax.dot_general(
            k_ref[pl.ds(begin, chunk), :],
            q,
            (((1,), (1,)), ((), ())),
            preferred_element_type=jnp.float32,
        )
        if masked:
            key_place = begin + lax.broadcasted_iota(jnp.int32, scores.shape, 0)
            scores = jnp.where(place_ref[0:1, :] >= key_place, scores, MASKED)
        old_max = max_ref[0:1, :]
        top = jnp.max(folded(scores, jnp.max), axis=0, keepdims=True) * EXP2_SCALE
        new_max = jnp.maximum(top, old_max)
        factor = jnp.exp2(old_max - new_max)
        weights = jnp.exp2(scores * EXP2_SCALE - new_max)
        total_ref[...] = total_ref[...] * factor + folded(weights, jnp.sum)
        update = lax.dot_general(
            v_ref[pl.ds(begin, chunk), :],
            weights.astype(jnp.bfloat16),
            (((0,), (0,)), ((), ())),
            preferred_element_type=jnp.float32,
        )
        acc_ref[...] = acc_ref[...] * factor + update
        max_ref[...] = jnp.broadcast_to(new_max, max_ref.shape)

    @pl.loop(0, span_ref[0])
    def _(index):
        absorb(index, False)

    @pl.loop(span_ref[0], span_ref[1])
    def _(index):
        absorb(index, True)

    out = acc_ref[...] / jnp.sum(total_ref[...], axis=0, keepdims=True)
    turned = out.T.astype(jnp.bfloat16)
    for j in range(rows // row_count):
        out_ref[:, j * HEAD_WIDTH : (j + 1) * HEAD_WIDTH] = turned[
            j * row_count : (j + 1) * row_count
        ]


def attend(span, places, queries, keys_values, first_head, head_count, chunk):
    row_count, features = queries.shape
    key_count, both = keys_values.shape
    kv_heads = both // (2 * HEAD_WIDTH)
    group_features = features // kv_heads
    heads = group_features // HEAD_WIDTH
    rows = row_count * heads
    pairs = rows * head_count * key_count
    place_rows = jnp.broadcast_to(jnp.tile(places, heads)[None, :], (8, rows))
    return pl.pallas_call(
        functools.partial(attend_kernel, chunk=chunk),
        grid=(head_count,),
        in_specs=[
            pl.BlockSpec(memory_space=pltpu.SMEM),
            pl.BlockSpec((8, rows), lambda g: (0, 0)),
            pl.BlockSpec((row_count, group_features), lambda g: (0, first_head + g)),
            pl.BlockSpec((key_count, HEAD_WIDTH), lambda g: (0, first_head + g)),
            pl.BlockSpec((key_count, HEAD_WIDTH), lambda g: (0, kv_heads + first_head + g)),
        ],
        out_specs=pl.BlockSpec((row_count, group_features), lambda g: (0, g)),
        out_shape=jax.ShapeDtypeStruct((row_count, group_features * head_count), jnp.bfloat16),
        scratch_shapes=[
            pltpu.VMEM((HEAD_WIDTH, rows), jnp.float32),
            pltpu.VMEM((8, rows), jnp.float32),
            pltpu.VMEM((8, rows), jnp.float32),
        ],
        compiler_params=pltpu.CompilerParams(vmem_limit_bytes=32 * 1024 * 1024),
        cost_estimate=pl.CostEstimate(
            flops=pairs * HEAD_WIDTH * 4, transcendentals=pairs, bytes_accessed=pairs
        ),
        name="attend",
        interpret=INTERPRET,
    )(span, place_rows, queries, keys_values, keys_values)


def attend_routed_kernel(place_ref, q_ref, k_ref, v_ref, out_ref):
    row_count = q_ref.shape[0]
    q = heads_to_rows(q_ref[...])
    scores = lax.dot_general(
        q, k_ref[...], (((1,), (1,)), ((), ())), preferred_element_type=jnp.float32
    )
    key_place = lax.broadcasted_iota(jnp.int32, scores.shape, 1)
    scores = jnp.where(place_ref[:, 0:1] >= key_place, scores, MASKED)
    top = jnp.max(scores, axis=1, keepdims=True) * EXP2_SCALE
    weights = jnp.exp2(scores * EXP2_SCALE - top)
    total = jnp.sum(weights, axis=1, keepdims=True)
    acc = jnp.dot(weights.astype(jnp.bfloat16), v_ref[...], preferred_element_type=jnp.float32)
    out = (acc / total).astype(jnp.bfloat16)
    for j in range(out.shape[0] // row_count):
        out_ref[:, j * HEAD_WIDTH : (j + 1) * HEAD_WIDTH] = out[
            j * row_count : (j + 1) * row_count
        ]


def attend_routed(places, queries, keys_values):
    row_count, features = queries.shape
    key_count, both = keys_values.shape
    kv_heads = both // (2 * HEAD_WIDTH)
    group_features = features // kv_heads
    heads = group_features // HEAD_WIDTH
    rows = row_count * heads
    pairs = rows * kv_heads * key_count
    place_rows = jnp.broadcast_to(jnp.tile(places, heads)[:, None], (rows, HEAD_WIDTH))
    return pl.pallas_call(
        attend_routed_kernel,
        grid=(kv_heads,),
        in_specs=[
            pl.BlockSpec((rows, HEAD_WIDTH), lambda g: (0, 0)),
            pl.BlockSpec((row_count, group_features), lambda g: (0, g)),
            pl.BlockSpec((key_count, HEAD_WIDTH), lambda g: (0, g)),
            pl.BlockSpec((key_count, HEAD_WIDTH), lambda g: (0, kv_heads + g)),
        ],
        out_specs=pl.BlockSpec((row_count, group_features), lambda g: (0, g)),
        out_shape=jax.ShapeDtypeStruct((row_count, features), jnp.bfloat16),
        compiler_params=pltpu.CompilerParams(vmem_limit_bytes=56 * 1024 * 1024),
        cost_estimate=pl.CostEstimate(
            flops=pairs * HEAD_WIDTH * 4, transcendentals=pairs, bytes_accessed=pairs
        ),
        name="attend_routed",
        interpret=INTERPRET,
    )(place_rows, queries, keys_values, keys_values)


def expert_in_kernel(*refs, piece_count):
    pieces = refs[:piece_count]
    gate_ref, up_ref, router_ref, own_ref, sent_ref = refs[piece_count:]
    members = jnp.concatenate([r[...] for r in pieces], axis=0)
    hidden_width = gate_ref.shape[1]
    for k, w_ref in enumerate((gate_ref, up_ref, router_ref)):
        part = jnp.dot(members, w_ref[...], preferred_element_type=jnp.float32)
        own_ref[:, k * hidden_width : (k + 1) * hidden_width] = part
        sent_ref[:, k * hidden_width : (k + 1) * hidden_width] = part.astype(jnp.bfloat16)


def expert_out_kernel(own_ref, other_ref, down_ref, out_ref):
    both = own_ref[...] + other_ref[...].astype(jnp.float32)
    hidden_width = down_ref.shape[0]
    gate = both[:, :hidden_width]
    up = both[:, hidden_width : 2 * hidden_width]
    score = both[:, 2 * hidden_width :]
    weight = 1.0 / (1.0 + jnp.exp(-score))
    gated = weight * gate
    hidden = (gated / (1.0 + jnp.exp(-gated)) * (weight * up)).astype(jnp.bfloat16)
    out_ref[...] = jnp.dot(hidden, down_ref[...], preferred_element_type=jnp.float32).astype(
        jnp.bfloat16
    )


def summed(*parts):
    total = parts[0].astype(jnp.float32)
    for part in parts[1:]:
        total = total + part.astype(jnp.float32)
    return total.astype(jnp.bfloat16)


def shards(queries, keys, values, expert_ids, router, w_gate, w_up, w_down):
    row_count, features = queries.shape[1:]
    ep_count = lax.axis_size("ep")
    far_count = lax.axis_size("far")
    near_count = lax.axis_size("near")
    ctx_count = far_count * near_count
    place = lax.axis_index(CTX)

    def shift(value, step):
        return lax.ppermute(
            value, CTX, [(i, (i + step) % ctx_count) for i in range(ctx_count)]
        )

    chosen = expert_ids[0, :, 0]
    choose = (chosen[:, None] == jnp.arange(ep_count, dtype=jnp.int32)[None, :]).astype(jnp.int32)
    earlier = jnp.cumsum(choose, axis=0) - choose
    slot_index = jnp.sum(earlier * choose, axis=1)
    target = chosen * CAP + slot_index
    spread = (target[None, :] == jnp.arange(ep_count * CAP, dtype=jnp.int32)[:, None]).astype(
        jnp.bfloat16
    )
    hidden_width = w_gate.shape[2]
    kv_heads = keys.shape[2] // HEAD_WIDTH
    router_wide = jnp.broadcast_to(router, (features, hidden_width))

    q = queries[0]
    own_kv = jnp.concatenate([keys[0], values[0]], axis=1)
    keys_values = lax.all_gather(own_kv, CTX, axis=0, tiled=True)
    key_count = keys_values.shape[0]
    own_chunk = min(OWN_CHUNK, key_count)

    routed_q = jnp.dot(spread, q, preferred_element_type=jnp.float32).astype(jnp.bfloat16)
    routed_row = jnp.sum(
        spread.astype(jnp.float32) * jnp.arange(row_count, dtype=jnp.float32)[None, :],
        axis=1,
        keepdims=True,
    )
    sent_q = jnp.concatenate(
        [routed_q, jnp.broadcast_to(routed_row, (ep_count * CAP, HEAD_WIDTH)).astype(jnp.bfloat16)],
        axis=1,
    )
    far_q = lax.all_gather(sent_q, "far", axis=0)
    far_q = far_q.reshape(far_count, ep_count, CAP, features + HEAD_WIDTH)
    far_q = jnp.transpose(far_q, (1, 0, 2, 3)).reshape(-1, features + HEAD_WIDTH)
    set_q = far_q[:, :features]
    in_device = far_q[:, features].astype(jnp.int32)
    far_of = (jnp.arange(set_q.shape[0], dtype=jnp.int32) // CAP) % far_count
    set_places = (far_of * near_count + lax.axis_index("near")) * row_count + in_device
    set_attended = attend_routed(set_places, set_q, keys_values)
    arrived = lax.all_to_all(
        set_attended.reshape(ep_count, far_count * CAP, features), "ep", 0, 0, tiled=True
    )
    own_set = arrived.reshape(ep_count * far_count * CAP, features)

    first_chunk = place * row_count // own_chunk
    own_span = jnp.stack([first_chunk, first_chunk + 1]).astype(jnp.int32)
    own_places = place * row_count + jnp.arange(row_count, dtype=jnp.int32)

    ahead_count = near_count // 2
    back_count = near_count - 1 - ahead_count
    ahead = back = own_set
    ahead_pieces, back_pieces = [], []
    for step in range(1, ahead_count + 1):
        ahead = shift(ahead, 1)
        ahead_pieces.append(ahead)
        if step <= back_count:
            back = shift(back, -1)
            back_pieces.append(back)
    pieces = [own_set] + ahead_pieces + back_pieces
    set_rows = own_set.shape[0]
    member_rows = set_rows * near_count

    own_part, sent_part = pl.pallas_call(
        functools.partial(expert_in_kernel, piece_count=near_count),
        out_shape=[
            jax.ShapeDtypeStruct((member_rows, 3 * hidden_width), jnp.float32),
            jax.ShapeDtypeStruct((member_rows, 3 * hidden_width), jnp.bfloat16),
        ],
        compiler_params=pltpu.CompilerParams(vmem_limit_bytes=24 * 1024 * 1024),
        name="expert_in",
        interpret=INTERPRET,
    )(*pieces, w_gate[0], w_up[0], router_wide)
    other_part = lax.ppermute(sent_part, "tp", [(0, 1), (1, 0)])
    partial_out = pl.pallas_call(
        expert_out_kernel,
        out_shape=jax.ShapeDtypeStruct((member_rows, features), jnp.bfloat16),
        compiler_params=pltpu.CompilerParams(vmem_limit_bytes=24 * 1024 * 1024),
        name="expert_out",
        interpret=INTERPRET,
    )(own_part, other_part, w_down[0])
    parts = [partial_out[k * set_rows : (k + 1) * set_rows] for k in range(near_count)]
    own_out = parts[0]
    ahead_out = parts[1 : 1 + ahead_count]
    back_out = parts[1 + ahead_count :]

    ahead_sum, back_sum = None, None
    for step in range(ahead_count, 0, -1):
        mine = ahead_out[step - 1]
        ahead_sum = shift(mine if ahead_sum is None else summed(mine, ahead_sum), -1)
        if step <= back_count:
            mine = back_out[step - 1]
            back_sum = shift(mine if back_sum is None else summed(mine, back_sum), 1)
    set_sum = summed(own_out, ahead_sum, back_sum)
    set_sum, q = lax.optimization_barrier((set_sum, q))
    attended = attend(own_span, own_places, q, keys_values, 0, kv_heads, own_chunk)
    returned = lax.all_to_all(
        set_sum.reshape(ep_count * far_count, CAP, features), ("ep", "far"), 0, 0, tiled=True
    )
    expert_rows = jnp.sum(
        returned.reshape(ep_count, far_count, CAP, features).astype(jnp.float32), axis=1
    ).astype(jnp.bfloat16).reshape(ep_count * CAP, features)
    routed = lax.dot_general(
        spread, expert_rows, (((0,), (0,)), ((), ())), preferred_element_type=jnp.float32
    )
    layer_out = (attended.astype(jnp.float32) + routed).astype(jnp.bfloat16)
    return layer_out[None]


def solution(mesh):
    shape = dict(zip(mesh.axis_names, mesh.devices.shape))
    near = NEAR if shape["ctx"] % NEAR == 0 else shape["ctx"]
    names, sizes = [], []
    for name in mesh.axis_names:
        if name == "ctx":
            names += ["far", "near"]
            sizes += [shape[name] // near, near]
        else:
            names.append(name)
            sizes.append(shape[name])
    split = Mesh(mesh.devices.reshape(sizes), tuple(names))
    placed = (
        P(("groups", "ep"), CTX, "tp"),
        P(("groups", "ep"), CTX, "tp"),
        P(("groups", "ep"), CTX, "tp"),
        P(("groups", "ep"), CTX, None),
        P("tp", "ep"),
        P("ep", "tp", CTX),
        P("ep", "tp", CTX),
        P("ep", CTX, "tp"),
    )
    return jax.shard_map(
        shards,
        mesh=split,
        in_specs=placed,
        out_specs=P(("groups", "ep"), CTX, "tp"),
        check_vma=False,
    )
```

```python
import functools

import jax
import jax.numpy as jnp
from jax import lax
from jax.experimental import pallas as pl
from jax.experimental.pallas import tpu as pltpu
from jax.sharding import Mesh, PartitionSpec as P

HEAD_WIDTH = 128
CAP = 2
NEAR = 8
CTX = ("far", "near")
MASKED = -1e30
EXP2_SCALE = HEAD_WIDTH ** (-0.5) * 1.4426950408889634
OWN_CHUNK = 1024
EARLY_HEADS = 2
INTERPRET = False


def heads_to_rows(block):
    heads = block.shape[1] // HEAD_WIDTH
    return jnp.concatenate(
        [block[:, j * HEAD_WIDTH : (j + 1) * HEAD_WIDTH] for j in range(heads)], axis=0
    )


def attend_kernel(
    span_ref, place_ref, q_ref, k_ref, v_ref, out_ref, acc_ref, max_ref, total_ref, *, chunk
):
    row_count = q_ref.shape[0]
    q = heads_to_rows(q_ref[...])
    rows = q.shape[0]
    acc_ref[...] = jnp.zeros(acc_ref.shape, jnp.float32)
    max_ref[...] = jnp.full(max_ref.shape, MASKED, jnp.float32)
    total_ref[...] = jnp.zeros(total_ref.shape, jnp.float32)

    def folded(piece, reduce):
        return reduce(piece.reshape(chunk // 8, 8, rows), axis=0)

    def absorb(index, masked):
        begin = pl.multiple_of(index * chunk, chunk)
        scores = lax.dot_general(
            k_ref[pl.ds(begin, chunk), :],
            q,
            (((1,), (1,)), ((), ())),
            preferred_element_type=jnp.float32,
        )
        if masked:
            key_place = begin + lax.broadcasted_iota(jnp.int32, scores.shape, 0)
            scores = jnp.where(place_ref[0:1, :] >= key_place, scores, MASKED)
        old_max = max_ref[0:1, :]
        top = jnp.max(folded(scores, jnp.max), axis=0, keepdims=True) * EXP2_SCALE
        new_max = jnp.maximum(top, old_max)
        factor = jnp.exp2(old_max - new_max)
        weights = jnp.exp2(scores * EXP2_SCALE - new_max)
        total_ref[...] = total_ref[...] * factor + folded(weights, jnp.sum)
        update = lax.dot_general(
            v_ref[pl.ds(begin, chunk), :],
            weights.astype(jnp.bfloat16),
            (((0,), (0,)), ((), ())),
            preferred_element_type=jnp.float32,
        )
        acc_ref[...] = acc_ref[...] * factor + update
        max_ref[...] = jnp.broadcast_to(new_max, max_ref.shape)

    @pl.loop(0, span_ref[0])
    def _(index):
        absorb(index, False)

    @pl.loop(span_ref[0], span_ref[1])
    def _(index):
        absorb(index, True)

    out = acc_ref[...] / jnp.sum(total_ref[...], axis=0, keepdims=True)
    turned = out.T.astype(jnp.bfloat16)
    for j in range(rows // row_count):
        out_ref[:, j * HEAD_WIDTH : (j + 1) * HEAD_WIDTH] = turned[
            j * row_count : (j + 1) * row_count
        ]


def attend(span, places, queries, keys_values, first_head, head_count, chunk):
    row_count, features = queries.shape
    key_count, both = keys_values.shape
    kv_heads = both // (2 * HEAD_WIDTH)
    group_features = features // kv_heads
    heads = group_features // HEAD_WIDTH
    rows = row_count * heads
    pairs = rows * head_count * key_count
    place_rows = jnp.broadcast_to(jnp.tile(places, heads)[None, :], (8, rows))
    return pl.pallas_call(
        functools.partial(attend_kernel, chunk=chunk),
        grid=(head_count,),
        in_specs=[
            pl.BlockSpec(memory_space=pltpu.SMEM),
            pl.BlockSpec((8, rows), lambda g: (0, 0)),
            pl.BlockSpec((row_count, group_features), lambda g: (0, first_head + g)),
            pl.BlockSpec((key_count, HEAD_WIDTH), lambda g: (0, first_head + g)),
            pl.BlockSpec((key_count, HEAD_WIDTH), lambda g: (0, kv_heads + first_head + g)),
        ],
        out_specs=pl.BlockSpec((row_count, group_features), lambda g: (0, g)),
        out_shape=jax.ShapeDtypeStruct((row_count, group_features * head_count), jnp.bfloat16),
        scratch_shapes=[
            pltpu.VMEM((HEAD_WIDTH, rows), jnp.float32),
            pltpu.VMEM((8, rows), jnp.float32),
            pltpu.VMEM((8, rows), jnp.float32),
        ],
        compiler_params=pltpu.CompilerParams(vmem_limit_bytes=56 * 1024 * 1024),
        cost_estimate=pl.CostEstimate(
            flops=pairs * HEAD_WIDTH * 4, transcendentals=pairs, bytes_accessed=pairs
        ),
        name="attend",
        interpret=INTERPRET,
    )(span, place_rows, queries, keys_values, keys_values)


def attend_routed_kernel(begin_ref, row_ref, q_ref, k_ref, v_ref, out_ref, *, far_count):
    row_count = q_ref.shape[0]
    q = heads_to_rows(q_ref[...])
    begins = jnp.zeros(row_ref.shape, jnp.int32)
    far_of = (lax.broadcasted_iota(jnp.int32, row_ref.shape, 0) // CAP) % far_count
    for f in range(far_count):
        begins = jnp.where(far_of == f, begin_ref[f], begins)
    places = begins + row_ref[...].astype(jnp.float32).astype(jnp.int32)
    places = jnp.concatenate([places] * (q.shape[0] // row_count), axis=0)
    scores = lax.dot_general(
        q, k_ref[...], (((1,), (1,)), ((), ())), preferred_element_type=jnp.float32
    )
    key_place = lax.broadcasted_iota(jnp.int32, scores.shape, 1)
    scores = jnp.where(places[:, 0:1] >= key_place, scores, MASKED)
    top = jnp.max(scores, axis=1, keepdims=True) * EXP2_SCALE
    weights = jnp.exp2(scores * EXP2_SCALE - top)
    total = jnp.sum(weights, axis=1, keepdims=True)
    acc = jnp.dot(weights.astype(jnp.bfloat16), v_ref[...], preferred_element_type=jnp.float32)
    out = (acc / total).astype(jnp.bfloat16)
    for j in range(out.shape[0] // row_count):
        out_ref[:, j * HEAD_WIDTH : (j + 1) * HEAD_WIDTH] = out[
            j * row_count : (j + 1) * row_count
        ]


def attend_routed(begins, queries, keys_values):
    row_count, features = queries.shape
    features -= HEAD_WIDTH
    key_count, both = keys_values.shape
    kv_heads = both // (2 * HEAD_WIDTH)
    group_features = features // kv_heads
    pairs = row_count * features // HEAD_WIDTH * key_count
    return pl.pallas_call(
        functools.partial(attend_routed_kernel, far_count=begins.shape[0]),
        grid=(kv_heads,),
        in_specs=[
            pl.BlockSpec(memory_space=pltpu.SMEM),
            pl.BlockSpec((row_count, HEAD_WIDTH), lambda g: (0, features // HEAD_WIDTH)),
            pl.BlockSpec((row_count, group_features), lambda g: (0, g)),
            pl.BlockSpec((key_count, HEAD_WIDTH), lambda g: (0, g)),
            pl.BlockSpec((key_count, HEAD_WIDTH), lambda g: (0, kv_heads + g)),
        ],
        out_specs=pl.BlockSpec((row_count, group_features), lambda g: (0, g)),
        out_shape=jax.ShapeDtypeStruct((row_count, features), jnp.bfloat16),
        compiler_params=pltpu.CompilerParams(vmem_limit_bytes=56 * 1024 * 1024),
        cost_estimate=pl.CostEstimate(
            flops=pairs * HEAD_WIDTH * 4, transcendentals=pairs, bytes_accessed=pairs
        ),
        name="attend_routed",
        interpret=INTERPRET,
    )(begins, queries, queries, keys_values, keys_values)


def expert_in_kernel(*refs, piece_count):
    pieces = refs[:piece_count]
    gate_ref, up_ref, router_ref, own_ref, sent_ref = refs[piece_count:]
    members = jnp.concatenate([r[...] for r in pieces], axis=0)
    hidden_width = gate_ref.shape[1]
    router = jnp.broadcast_to(router_ref[...], (hidden_width, members.shape[1]))
    parts = (
        jnp.dot(members, gate_ref[...], preferred_element_type=jnp.float32),
        jnp.dot(members, up_ref[...], preferred_element_type=jnp.float32),
        lax.dot_general(
            members, router, (((1,), (1,)), ((), ())), preferred_element_type=jnp.float32
        ),
    )
    for k, part in enumerate(parts):
        own_ref[:, k * hidden_width : (k + 1) * hidden_width] = part
        sent_ref[:, k * hidden_width : (k + 1) * hidden_width] = part.astype(jnp.bfloat16)


def expert_out_kernel(own_ref, other_ref, down_ref, out_ref):
    both = own_ref[...] + other_ref[...].astype(jnp.float32)
    hidden_width = down_ref.shape[0]
    gate = both[:, :hidden_width]
    up = both[:, hidden_width : 2 * hidden_width]
    score = both[:, 2 * hidden_width :]
    weight = 1.0 / (1.0 + jnp.exp(-score))
    gated = weight * gate
    hidden = (gated / (1.0 + jnp.exp(-gated)) * (weight * up)).astype(jnp.bfloat16)
    out_ref[...] = jnp.dot(hidden, down_ref[...], preferred_element_type=jnp.float32).astype(
        jnp.bfloat16
    )


def summed(*parts):
    total = parts[0].astype(jnp.float32)
    for part in parts[1:]:
        total = total + part.astype(jnp.float32)
    return total.astype(jnp.bfloat16)


def shards(queries, keys, values, expert_ids, router, w_gate, w_up, w_down):
    row_count, features = queries.shape[1:]
    ep_count = lax.axis_size("ep")
    far_count = lax.axis_size("far")
    near_count = lax.axis_size("near")
    ctx_count = far_count * near_count
    place = lax.axis_index(CTX)

    def shift(value, step):
        return lax.ppermute(
            value, CTX, [(i, (i + step) % ctx_count) for i in range(ctx_count)]
        )

    chosen = expert_ids[0, :, 0]
    choose = (chosen[:, None] == jnp.arange(ep_count, dtype=jnp.int32)[None, :]).astype(jnp.int32)
    earlier = jnp.cumsum(choose, axis=0) - choose
    slot_index = jnp.sum(earlier * choose, axis=1)
    target = chosen * CAP + slot_index
    spread = (target[None, :] == jnp.arange(ep_count * CAP, dtype=jnp.int32)[:, None]).astype(
        jnp.bfloat16
    )
    hidden_width = w_gate.shape[2]
    kv_heads = keys.shape[2] // HEAD_WIDTH

    q = queries[0]
    own_kv = jnp.concatenate([keys[0], values[0]], axis=1)
    keys_values = lax.all_gather(own_kv, CTX, axis=0, tiled=True)
    key_count = keys_values.shape[0]
    own_chunk = min(OWN_CHUNK, key_count)

    routed_q = jnp.dot(spread, q, preferred_element_type=jnp.float32).astype(jnp.bfloat16)
    routed_row = jnp.sum(
        spread.astype(jnp.float32) * jnp.arange(row_count, dtype=jnp.float32)[None, :],
        axis=1,
        keepdims=True,
    )
    sent_q = jnp.concatenate(
        [routed_q, jnp.broadcast_to(routed_row, (ep_count * CAP, HEAD_WIDTH)).astype(jnp.bfloat16)],
        axis=1,
    )
    far_q = lax.all_gather(sent_q, "far", axis=0)
    far_q = far_q.reshape(far_count, ep_count, CAP, features + HEAD_WIDTH)
    far_q = jnp.transpose(far_q, (1, 0, 2, 3)).reshape(-1, features + HEAD_WIDTH)
    begins = (
        jnp.arange(far_count, dtype=jnp.int32) * near_count + lax.axis_index("near")
    ) * row_count
    set_attended = attend_routed(begins, far_q, keys_values)
    arrived = lax.all_to_all(
        set_attended.reshape(ep_count, far_count * CAP, features), "ep", 0, 0, tiled=True
    )
    own_set = arrived.reshape(ep_count * far_count * CAP, features)

    first_chunk = place * row_count // own_chunk
    own_span = jnp.stack([first_chunk, first_chunk + 1]).astype(jnp.int32)
    own_places = place * row_count + jnp.arange(row_count, dtype=jnp.int32)

    ahead_count = near_count // 2
    back_count = near_count - 1 - ahead_count
    ahead = back = own_set
    ahead_pieces, back_pieces = [], []
    for step in range(1, ahead_count + 1):
        ahead = shift(ahead, 1)
        ahead_pieces.append(ahead)
        if step <= back_count:
            back = shift(back, -1)
            back_pieces.append(back)
    pieces = [own_set] + ahead_pieces + back_pieces
    set_rows = own_set.shape[0]
    member_rows = set_rows * near_count

    own_part, sent_part = pl.pallas_call(
        functools.partial(expert_in_kernel, piece_count=near_count),
        out_shape=[
            jax.ShapeDtypeStruct((member_rows, 3 * hidden_width), jnp.float32),
            jax.ShapeDtypeStruct((member_rows, 3 * hidden_width), jnp.bfloat16),
        ],
        compiler_params=pltpu.CompilerParams(vmem_limit_bytes=24 * 1024 * 1024),
        name="expert_in",
        interpret=INTERPRET,
    )(*pieces, w_gate[0], w_up[0], router.reshape(1, features))
    other_part = lax.ppermute(sent_part, "tp", [(0, 1), (1, 0)])
    partial_out = pl.pallas_call(
        expert_out_kernel,
        out_shape=jax.ShapeDtypeStruct((member_rows, features), jnp.bfloat16),
        compiler_params=pltpu.CompilerParams(vmem_limit_bytes=24 * 1024 * 1024),
        name="expert_out",
        interpret=INTERPRET,
    )(own_part, other_part, w_down[0])
    partial_out, own_q = lax.optimization_barrier((partial_out, q))
    parts = [partial_out[k * set_rows : (k + 1) * set_rows] for k in range(near_count)]
    own_out = parts[0]
    ahead_out = parts[1 : 1 + ahead_count]
    back_out = parts[1 + ahead_count :]
    own_pieces = []
    early = min(EARLY_HEADS, kv_heads - 1)
    ahead_sum, back_sum = ahead_out[-1], back_out[-1]
    for step in range(ahead_count):
        ahead_sum = shift(ahead_sum, -1)
        if step < back_count:
            back_sum = shift(back_sum, 1)
        together = [ahead_sum, back_sum, own_q]
        if len(own_pieces) < early:
            together.append(
                attend(own_span, own_places, own_q, keys_values, len(own_pieces), 1, own_chunk)
            )
        ahead_sum, back_sum, own_q, *piece = lax.optimization_barrier(tuple(together))
        own_pieces += piece
        if step < ahead_count - 1:
            ahead_sum = summed(ahead_out[ahead_count - 2 - step], ahead_sum)
        if step < back_count - 1:
            back_sum = summed(back_out[back_count - 2 - step], back_sum)
    set_sum = summed(own_out, ahead_sum, back_sum)
    set_sum, own_q = lax.optimization_barrier((set_sum, own_q))
    own_pieces.append(
        attend(own_span, own_places, own_q, keys_values, early, kv_heads - early, own_chunk)
    )
    attended = jnp.concatenate(own_pieces, axis=1)
    returned = lax.all_to_all(
        set_sum.reshape(ep_count * far_count, CAP, features), ("ep", "far"), 0, 0, tiled=True
    )
    expert_rows = jnp.sum(
        returned.reshape(ep_count, far_count, CAP, features).astype(jnp.float32), axis=1
    ).astype(jnp.bfloat16).reshape(ep_count * CAP, features)
    routed = lax.dot_general(
        spread, expert_rows, (((0,), (0,)), ((), ())), preferred_element_type=jnp.float32
    )
    layer_out = (attended.astype(jnp.float32) + routed).astype(jnp.bfloat16)
    return layer_out[None]


def solution(mesh):
    shape = dict(zip(mesh.axis_names, mesh.devices.shape))
    near = NEAR if shape["ctx"] % NEAR == 0 else shape["ctx"]
    names, sizes = [], []
    for name in mesh.axis_names:
        if name == "ctx":
            names += ["far", "near"]
            sizes += [shape[name] // near, near]
        else:
            names.append(name)
            sizes.append(shape[name])
    split = Mesh(mesh.devices.reshape(sizes), tuple(names))
    placed = (
        P(("groups", "ep"), CTX, "tp"),
        P(("groups", "ep"), CTX, "tp"),
        P(("groups", "ep"), CTX, "tp"),
        P(("groups", "ep"), CTX, None),
        P("tp", "ep"),
        P("ep", "tp", CTX),
        P("ep", "tp", CTX),
        P("ep", CTX, "tp"),
    )
    return jax.shard_map(
        shards,
        mesh=split,
        in_specs=placed,
        out_specs=P(("groups", "ep"), CTX, "tp"),
        check_vma=False,
    )
```

```python
import functools

import jax
import jax.numpy as jnp
from jax import lax
from jax.experimental import pallas as pl
from jax.experimental.pallas import tpu as pltpu
from jax.sharding import Mesh, PartitionSpec as P

HEAD_WIDTH = 128
CAP = 2
NEAR = 8
CTX = ("far", "near")
MASKED = -1e30
EXP2_SCALE = HEAD_WIDTH ** (-0.5) * 1.4426950408889634
OWN_CHUNK = 2048
INTERPRET = False


def heads_to_rows(block):
    heads = block.shape[1] // HEAD_WIDTH
    return jnp.concatenate(
        [block[:, j * HEAD_WIDTH : (j + 1) * HEAD_WIDTH] for j in range(heads)], axis=0
    )


def attend_kernel(
    span_ref, q_ref, k_ref, v_ref, out_ref, score_ref, top_ref, total_ref, acc_ref, *, chunk
):
    row_count = q_ref.shape[0]
    q = heads_to_rows(q_ref[...])
    rows = q.shape[0]
    tiles = chunk // HEAD_WIDTH
    full = span_ref[0]

    def score(index, masked):
        begin = pl.multiple_of(index * chunk, chunk)
        scores = lax.dot_general(
            q,
            k_ref[pl.ds(begin, chunk), :],
            (((1,), (1,)), ((), ())),
            preferred_element_type=jnp.float32,
        )
        if masked:
            key_place = begin + lax.broadcasted_iota(jnp.int32, scores.shape, 1)
            row_place = lax.broadcasted_iota(jnp.int32, scores.shape, 0) % row_count
            scores = jnp.where(span_ref[1] + row_place >= key_place, scores, MASKED)
        score_ref[index] = scores
        top = top_ref[...]
        for t in range(tiles):
            top = jnp.maximum(top, scores[:, t * HEAD_WIDTH : (t + 1) * HEAD_WIDTH])
        top_ref[...] = top

    top_ref[...] = jnp.full(top_ref.shape, MASKED, jnp.float32)

    @pl.loop(0, full)
    def _(index):
        score(index, False)

    score(full, True)
    row_top = jnp.max(top_ref[...], axis=1, keepdims=True) * EXP2_SCALE
    top_ref[...] = jnp.broadcast_to(row_top, top_ref.shape)
    total_ref[...] = jnp.zeros(total_ref.shape, jnp.float32)
    acc_ref[...] = jnp.zeros(acc_ref.shape, jnp.float32)

    @pl.loop(0, full + 1)
    def _(index):
        begin = pl.multiple_of(index * chunk, chunk)
        top = top_ref[...]
        total = total_ref[...]
        weights = []
        for t in range(tiles):
            piece = score_ref[index, :, t * HEAD_WIDTH : (t + 1) * HEAD_WIDTH]
            weight = jnp.exp2(piece * EXP2_SCALE - top)
            total = total + weight
            weights.append(weight.astype(jnp.bfloat16))
        total_ref[...] = total
        acc_ref[...] += jnp.dot(
            jnp.concatenate(weights, axis=1),
            v_ref[pl.ds(begin, chunk), :],
            preferred_element_type=jnp.float32,
        )

    out = acc_ref[...] / jnp.sum(total_ref[...], axis=1, keepdims=True)
    out = out.astype(jnp.bfloat16)
    for j in range(rows // row_count):
        out_ref[:, j * HEAD_WIDTH : (j + 1) * HEAD_WIDTH] = out[
            j * row_count : (j + 1) * row_count
        ]


def attend(span, queries, keys_values, first_head, head_count, chunk):
    row_count, features = queries.shape
    key_count, both = keys_values.shape
    kv_heads = both // (2 * HEAD_WIDTH)
    group_features = features // kv_heads
    rows = row_count * group_features // HEAD_WIDTH
    pairs = rows * head_count * key_count
    return pl.pallas_call(
        functools.partial(attend_kernel, chunk=chunk),
        grid=(head_count,),
        in_specs=[
            pl.BlockSpec(memory_space=pltpu.SMEM),
            pl.BlockSpec((row_count, group_features), lambda g: (0, first_head + g)),
            pl.BlockSpec((key_count, HEAD_WIDTH), lambda g: (0, first_head + g)),
            pl.BlockSpec((key_count, HEAD_WIDTH), lambda g: (0, kv_heads + first_head + g)),
        ],
        out_specs=pl.BlockSpec((row_count, group_features), lambda g: (0, g)),
        out_shape=jax.ShapeDtypeStruct((row_count, group_features * head_count), jnp.bfloat16),
        scratch_shapes=[pltpu.VMEM((key_count // chunk, rows, chunk), jnp.float32)]
        + [pltpu.VMEM((rows, HEAD_WIDTH), jnp.float32)] * 3,
        compiler_params=pltpu.CompilerParams(vmem_limit_bytes=56 * 1024 * 1024),
        cost_estimate=pl.CostEstimate(
            flops=pairs * HEAD_WIDTH * 4, transcendentals=pairs, bytes_accessed=pairs
        ),
        name="attend",
        interpret=INTERPRET,
    )(span, queries, keys_values, keys_values)


def attend_routed_kernel(begin_ref, row_ref, q_ref, k_ref, v_ref, out_ref, *, far_count):
    row_count = q_ref.shape[0]
    q = heads_to_rows(q_ref[...])
    begins = jnp.zeros(row_ref.shape, jnp.int32)
    far_of = (lax.broadcasted_iota(jnp.int32, row_ref.shape, 0) // CAP) % far_count
    for f in range(far_count):
        begins = jnp.where(far_of == f, begin_ref[f], begins)
    places = begins + row_ref[...].astype(jnp.float32).astype(jnp.int32)
    places = jnp.concatenate([places] * (q.shape[0] // row_count), axis=0)
    scores = lax.dot_general(
        q, k_ref[...], (((1,), (1,)), ((), ())), preferred_element_type=jnp.float32
    )
    key_place = lax.broadcasted_iota(jnp.int32, scores.shape, 1)
    scores = jnp.where(places[:, 0:1] >= key_place, scores, MASKED)
    top = jnp.max(scores, axis=1, keepdims=True) * EXP2_SCALE
    weights = jnp.exp2(scores * EXP2_SCALE - top)
    total = jnp.sum(weights, axis=1, keepdims=True)
    acc = jnp.dot(weights.astype(jnp.bfloat16), v_ref[...], preferred_element_type=jnp.float32)
    out = (acc / total).astype(jnp.bfloat16)
    for j in range(out.shape[0] // row_count):
        out_ref[:, j * HEAD_WIDTH : (j + 1) * HEAD_WIDTH] = out[
            j * row_count : (j + 1) * row_count
        ]


def attend_routed(begins, queries, keys_values):
    row_count, features = queries.shape
    features -= HEAD_WIDTH
    key_count, both = keys_values.shape
    kv_heads = both // (2 * HEAD_WIDTH)
    group_features = features // kv_heads
    pairs = row_count * features // HEAD_WIDTH * key_count
    return pl.pallas_call(
        functools.partial(attend_routed_kernel, far_count=begins.shape[0]),
        grid=(kv_heads,),
        in_specs=[
            pl.BlockSpec(memory_space=pltpu.SMEM),
            pl.BlockSpec((row_count, HEAD_WIDTH), lambda g: (0, features // HEAD_WIDTH)),
            pl.BlockSpec((row_count, group_features), lambda g: (0, g)),
            pl.BlockSpec((key_count, HEAD_WIDTH), lambda g: (0, g)),
            pl.BlockSpec((key_count, HEAD_WIDTH), lambda g: (0, kv_heads + g)),
        ],
        out_specs=pl.BlockSpec((row_count, group_features), lambda g: (0, g)),
        out_shape=jax.ShapeDtypeStruct((row_count, features), jnp.bfloat16),
        compiler_params=pltpu.CompilerParams(vmem_limit_bytes=56 * 1024 * 1024),
        cost_estimate=pl.CostEstimate(
            flops=pairs * HEAD_WIDTH * 4, transcendentals=pairs, bytes_accessed=pairs
        ),
        name="attend_routed",
        interpret=INTERPRET,
    )(begins, queries, queries, keys_values, keys_values)


def expert_in_kernel(*refs, piece_count):
    halves = refs[piece_count : piece_count + 2]
    gate_ref, up_ref, router_ref, own_ref, sent_ref = refs[piece_count + 2 :]
    far_set = jnp.concatenate([r[...] for r in halves], axis=1)
    members = jnp.concatenate([r[...] for r in refs[:piece_count]] + [far_set], axis=0)
    hidden_width = gate_ref.shape[1]
    router = jnp.broadcast_to(router_ref[...], (hidden_width, members.shape[1]))
    parts = (
        jnp.dot(members, gate_ref[...], preferred_element_type=jnp.float32),
        jnp.dot(members, up_ref[...], preferred_element_type=jnp.float32),
        lax.dot_general(
            members, router, (((1,), (1,)), ((), ())), preferred_element_type=jnp.float32
        ),
    )
    for k, part in enumerate(parts):
        own_ref[:, k * hidden_width : (k + 1) * hidden_width] = part
        sent_ref[:, k * hidden_width : (k + 1) * hidden_width] = part.astype(jnp.bfloat16)


def expert_out_kernel(own_ref, other_ref, down_ref, out_ref):
    both = own_ref[...] + other_ref[...].astype(jnp.float32)
    hidden_width = down_ref.shape[0]
    gate = both[:, :hidden_width]
    up = both[:, hidden_width : 2 * hidden_width]
    score = both[:, 2 * hidden_width :]
    weight = 1.0 / (1.0 + jnp.exp(-score))
    gated = weight * gate
    hidden = (gated / (1.0 + jnp.exp(-gated)) * (weight * up)).astype(jnp.bfloat16)
    out_ref[...] = jnp.dot(hidden, down_ref[...], preferred_element_type=jnp.float32).astype(
        jnp.bfloat16
    )


def summed(*parts):
    total = parts[0].astype(jnp.float32)
    for part in parts[1:]:
        total = total + part.astype(jnp.float32)
    return total.astype(jnp.bfloat16)


def shards(queries, keys, values, expert_ids, router, w_gate, w_up, w_down):
    row_count, features = queries.shape[1:]
    ep_count = lax.axis_size("ep")
    far_count = lax.axis_size("far")
    near_count = lax.axis_size("near")
    ctx_count = far_count * near_count
    place = lax.axis_index(CTX)

    def shift(value, step):
        return lax.ppermute(
            value, CTX, [(i, (i + step) % ctx_count) for i in range(ctx_count)]
        )

    chosen = expert_ids[0, :, 0]
    choose = (chosen[:, None] == jnp.arange(ep_count, dtype=jnp.int32)[None, :]).astype(jnp.int32)
    earlier = jnp.cumsum(choose, axis=0) - choose
    slot_index = jnp.sum(earlier * choose, axis=1)
    target = chosen * CAP + slot_index
    spread = (target[None, :] == jnp.arange(ep_count * CAP, dtype=jnp.int32)[:, None]).astype(
        jnp.bfloat16
    )
    hidden_width = w_gate.shape[2]
    kv_heads = keys.shape[2] // HEAD_WIDTH

    q = queries[0]
    own_kv = jnp.concatenate([keys[0], values[0]], axis=1)
    keys_values = lax.all_gather(own_kv, CTX, axis=0, tiled=True)
    key_count = keys_values.shape[0]
    own_chunk = min(OWN_CHUNK, key_count)

    routed_q = jnp.dot(spread, q, preferred_element_type=jnp.float32).astype(jnp.bfloat16)
    routed_row = jnp.sum(
        spread.astype(jnp.float32) * jnp.arange(row_count, dtype=jnp.float32)[None, :],
        axis=1,
        keepdims=True,
    )
    sent_q = jnp.concatenate(
        [routed_q, jnp.broadcast_to(routed_row, (ep_count * CAP, HEAD_WIDTH)).astype(jnp.bfloat16)],
        axis=1,
    )
    far_q = lax.all_gather(sent_q, "far", axis=0)
    far_q = far_q.reshape(far_count, ep_count, CAP, features + HEAD_WIDTH)
    far_q = jnp.transpose(far_q, (1, 0, 2, 3)).reshape(-1, features + HEAD_WIDTH)
    begins = (
        jnp.arange(far_count, dtype=jnp.int32) * near_count + lax.axis_index("near")
    ) * row_count
    set_attended = attend_routed(begins, far_q, keys_values)
    arrived = lax.all_to_all(
        set_attended.reshape(ep_count, far_count * CAP, features), "ep", 0, 0, tiled=True
    )
    own_set = arrived.reshape(ep_count * far_count * CAP, features)

    first_chunk = place * row_count // own_chunk
    own_span = jnp.stack([first_chunk, place * row_count]).astype(jnp.int32)

    side_count = near_count // 2 - 1
    half = features // 2
    ahead = back = own_set
    ahead_pieces, back_pieces = [], []
    for _ in range(side_count):
        ahead = shift(ahead, 1)
        ahead_pieces.append(ahead)
        back = shift(back, -1)
        back_pieces.append(back)
    halves = [shift(ahead[:, :half], 1), shift(back[:, half:], -1)]
    pieces = [own_set] + ahead_pieces + back_pieces
    set_rows = own_set.shape[0]
    member_rows = set_rows * near_count

    own_part, sent_part = pl.pallas_call(
        functools.partial(expert_in_kernel, piece_count=near_count - 1),
        out_shape=[
            jax.ShapeDtypeStruct((member_rows, 3 * hidden_width), jnp.float32),
            jax.ShapeDtypeStruct((member_rows, 3 * hidden_width), jnp.bfloat16),
        ],
        compiler_params=pltpu.CompilerParams(vmem_limit_bytes=24 * 1024 * 1024),
        name="expert_in",
        interpret=INTERPRET,
    )(*pieces, *halves, w_gate[0], w_up[0], router.reshape(1, features))
    other_part = lax.ppermute(sent_part, "tp", [(0, 1), (1, 0)])
    partial_out = pl.pallas_call(
        expert_out_kernel,
        out_shape=jax.ShapeDtypeStruct((member_rows, features), jnp.bfloat16),
        compiler_params=pltpu.CompilerParams(vmem_limit_bytes=24 * 1024 * 1024),
        name="expert_out",
        interpret=INTERPRET,
    )(own_part, other_part, w_down[0])
    parts = [partial_out[k * set_rows : (k + 1) * set_rows] for k in range(near_count)]
    own_out = parts[0]
    ahead_out = parts[1 : 1 + side_count]
    back_out = parts[1 + side_count : -1]
    ahead_half = shift(parts[-1][:, :half], -1)
    back_half = shift(parts[-1][:, half:], 1)
    mine, also = ahead_out[-1], back_out[-1]
    ahead_sum = jnp.concatenate([summed(mine[:, :half], ahead_half), mine[:, half:]], axis=1)
    back_sum = jnp.concatenate([also[:, :half], summed(also[:, half:], back_half)], axis=1)
    for step in range(side_count - 1, -1, -1):
        ahead_sum = shift(ahead_sum, -1)
        back_sum = shift(back_sum, 1)
        if step:
            ahead_sum = summed(ahead_out[step - 1], ahead_sum)
            back_sum = summed(back_out[step - 1], back_sum)
    set_sum = summed(own_out, ahead_sum, back_sum)
    set_sum, own_q = lax.optimization_barrier((set_sum, q))
    attended = attend(own_span, own_q, keys_values, 0, kv_heads, own_chunk)
    returned = lax.all_to_all(
        set_sum.reshape(ep_count * far_count, CAP, features), ("ep", "far"), 0, 0, tiled=True
    )
    expert_rows = jnp.sum(
        returned.reshape(ep_count, far_count, CAP, features).astype(jnp.float32), axis=1
    ).astype(jnp.bfloat16).reshape(ep_count * CAP, features)
    routed = lax.dot_general(
        spread, expert_rows, (((0,), (0,)), ((), ())), preferred_element_type=jnp.float32
    )
    layer_out = (attended.astype(jnp.float32) + routed).astype(jnp.bfloat16)
    return layer_out[None]


def solution(mesh):
    shape = dict(zip(mesh.axis_names, mesh.devices.shape))
    near = NEAR if shape["ctx"] % NEAR == 0 else shape["ctx"]
    names, sizes = [], []
    for name in mesh.axis_names:
        if name == "ctx":
            names += ["far", "near"]
            sizes += [shape[name] // near, near]
        else:
            names.append(name)
            sizes.append(shape[name])
    split = Mesh(mesh.devices.reshape(sizes), tuple(names))
    placed = (
        P(("groups", "ep"), CTX, "tp"),
        P(("groups", "ep"), CTX, "tp"),
        P(("groups", "ep"), CTX, "tp"),
        P(("groups", "ep"), CTX, None),
        P("tp", "ep"),
        P("ep", "tp", CTX),
        P("ep", "tp", CTX),
        P("ep", CTX, "tp"),
    )
    return jax.shard_map(
        shards,
        mesh=split,
        in_specs=placed,
        out_specs=P(("groups", "ep"), CTX, "tp"),
        check_vma=False,
    )
```

```python
import functools

import jax
import jax.numpy as jnp
from jax import lax
from jax.experimental import pallas as pl
from jax.experimental.pallas import tpu as pltpu
from jax.sharding import Mesh, PartitionSpec as P

HEAD_WIDTH = 128
CAP = 2
NEAR = 8
CTX = ("far", "near")
MASKED = -1e30
EXP2_SCALE = HEAD_WIDTH ** (-0.5) * 1.4426950408889634
OWN_CHUNK = 2048
INTERPRET = False


def heads_to_rows(block):
    heads = block.shape[1] // HEAD_WIDTH
    return jnp.concatenate(
        [block[:, j * HEAD_WIDTH : (j + 1) * HEAD_WIDTH] for j in range(heads)], axis=0
    )


def attend_kernel(
    span_ref, q_ref, k_ref, v_ref, out_ref, score_ref, top_ref, total_ref, acc_ref, *, chunk
):
    row_count = q_ref.shape[0]
    q = heads_to_rows(q_ref[...])
    rows = q.shape[0]
    tiles = chunk // HEAD_WIDTH
    full = span_ref[0]

    def score(index, masked):
        begin = pl.multiple_of(index * chunk, chunk)
        scores = lax.dot_general(
            q,
            k_ref[pl.ds(begin, chunk), :],
            (((1,), (1,)), ((), ())),
            preferred_element_type=jnp.float32,
        )
        if masked:
            key_place = begin + lax.broadcasted_iota(jnp.int32, scores.shape, 1)
            row_place = lax.broadcasted_iota(jnp.int32, scores.shape, 0) % row_count
            scores = jnp.where(span_ref[1] + row_place >= key_place, scores, MASKED)
        score_ref[index] = scores
        top = top_ref[...]
        for t in range(tiles):
            top = jnp.maximum(top, scores[:, t * HEAD_WIDTH : (t + 1) * HEAD_WIDTH])
        top_ref[...] = top

    top_ref[...] = jnp.full(top_ref.shape, MASKED, jnp.float32)

    @pl.loop(0, full)
    def _(index):
        score(index, False)

    score(full, True)
    row_top = jnp.max(top_ref[...], axis=1, keepdims=True) * EXP2_SCALE
    top_ref[...] = jnp.broadcast_to(row_top, top_ref.shape)
    total_ref[...] = jnp.zeros(total_ref.shape, jnp.float32)
    acc_ref[...] = jnp.zeros(acc_ref.shape, jnp.float32)

    @pl.loop(0, full + 1)
    def _(index):
        begin = pl.multiple_of(index * chunk, chunk)
        top = top_ref[...]
        total = total_ref[...]
        weights = []
        for t in range(tiles):
            piece = score_ref[index, :, t * HEAD_WIDTH : (t + 1) * HEAD_WIDTH]
            weight = jnp.exp2(piece * EXP2_SCALE - top)
            total = total + weight
            weights.append(weight.astype(jnp.bfloat16))
        total_ref[...] = total
        acc_ref[...] += jnp.dot(
            jnp.concatenate(weights, axis=1),
            v_ref[pl.ds(begin, chunk), :],
            preferred_element_type=jnp.float32,
        )

    out = acc_ref[...] / jnp.sum(total_ref[...], axis=1, keepdims=True)
    out = out.astype(jnp.bfloat16)
    for j in range(rows // row_count):
        out_ref[:, j * HEAD_WIDTH : (j + 1) * HEAD_WIDTH] = out[
            j * row_count : (j + 1) * row_count
        ]


def attend(span, queries, keys_values, first_head, head_count, chunk):
    row_count, features = queries.shape
    key_count, both = keys_values.shape
    kv_heads = both // (2 * HEAD_WIDTH)
    group_features = features // kv_heads
    rows = row_count * group_features // HEAD_WIDTH
    pairs = rows * head_count * key_count
    return pl.pallas_call(
        functools.partial(attend_kernel, chunk=chunk),
        grid=(head_count,),
        in_specs=[
            pl.BlockSpec(memory_space=pltpu.SMEM),
            pl.BlockSpec((row_count, group_features), lambda g: (0, first_head + g)),
            pl.BlockSpec((key_count, HEAD_WIDTH), lambda g: (0, first_head + g)),
            pl.BlockSpec((key_count, HEAD_WIDTH), lambda g: (0, kv_heads + first_head + g)),
        ],
        out_specs=pl.BlockSpec((row_count, group_features), lambda g: (0, g)),
        out_shape=jax.ShapeDtypeStruct((row_count, group_features * head_count), jnp.bfloat16),
        scratch_shapes=[pltpu.VMEM((key_count // chunk, rows, chunk), jnp.float32)]
        + [pltpu.VMEM((rows, HEAD_WIDTH), jnp.float32)] * 3,
        compiler_params=pltpu.CompilerParams(vmem_limit_bytes=50 * 1024 * 1024),
        cost_estimate=pl.CostEstimate(
            flops=pairs * HEAD_WIDTH * 4, transcendentals=pairs, bytes_accessed=pairs
        ),
        name="attend",
        interpret=INTERPRET,
    )(span, queries, keys_values, keys_values)


def attend_routed_kernel(begin_ref, row_ref, q_ref, k_ref, v_ref, out_ref, *, far_count):
    row_count = q_ref.shape[0]
    q = heads_to_rows(q_ref[...])
    begins = jnp.zeros(row_ref.shape, jnp.int32)
    far_of = (lax.broadcasted_iota(jnp.int32, row_ref.shape, 0) // CAP) % far_count
    for f in range(far_count):
        begins = jnp.where(far_of == f, begin_ref[f], begins)
    places = begins + row_ref[...].astype(jnp.float32).astype(jnp.int32)
    places = jnp.concatenate([places] * (q.shape[0] // row_count), axis=0)
    scores = lax.dot_general(
        q, k_ref[...], (((1,), (1,)), ((), ())), preferred_element_type=jnp.float32
    )
    key_place = lax.broadcasted_iota(jnp.int32, scores.shape, 1)
    scores = jnp.where(places[:, 0:1] >= key_place, scores, MASKED)
    top = jnp.max(scores, axis=1, keepdims=True) * EXP2_SCALE
    weights = jnp.exp2(scores * EXP2_SCALE - top)
    total = jnp.sum(weights, axis=1, keepdims=True)
    acc = jnp.dot(weights.astype(jnp.bfloat16), v_ref[...], preferred_element_type=jnp.float32)
    out = (acc / total).astype(jnp.bfloat16)
    for j in range(out.shape[0] // row_count):
        out_ref[:, j * HEAD_WIDTH : (j + 1) * HEAD_WIDTH] = out[
            j * row_count : (j + 1) * row_count
        ]


def attend_routed(begins, queries, keys_values):
    row_count, features = queries.shape
    features -= HEAD_WIDTH
    key_count, both = keys_values.shape
    kv_heads = both // (2 * HEAD_WIDTH)
    group_features = features // kv_heads
    pairs = row_count * features // HEAD_WIDTH * key_count
    return pl.pallas_call(
        functools.partial(attend_routed_kernel, far_count=begins.shape[0]),
        grid=(kv_heads,),
        in_specs=[
            pl.BlockSpec(memory_space=pltpu.SMEM),
            pl.BlockSpec((row_count, HEAD_WIDTH), lambda g: (0, features // HEAD_WIDTH)),
            pl.BlockSpec((row_count, group_features), lambda g: (0, g)),
            pl.BlockSpec((key_count, HEAD_WIDTH), lambda g: (0, g)),
            pl.BlockSpec((key_count, HEAD_WIDTH), lambda g: (0, kv_heads + g)),
        ],
        out_specs=pl.BlockSpec((row_count, group_features), lambda g: (0, g)),
        out_shape=jax.ShapeDtypeStruct((row_count, features), jnp.bfloat16),
        compiler_params=pltpu.CompilerParams(vmem_limit_bytes=50 * 1024 * 1024),
        cost_estimate=pl.CostEstimate(
            flops=pairs * HEAD_WIDTH * 4, transcendentals=pairs, bytes_accessed=pairs
        ),
        name="attend_routed",
        interpret=INTERPRET,
    )(begins, queries, queries, keys_values, keys_values)


def expert_in_kernel(*refs, piece_count):
    pieces = refs[:piece_count]
    gate_ref, up_ref, router_ref, own_ref, sent_ref = refs[piece_count:]
    members = jnp.concatenate([r[...] for r in pieces], axis=0)
    hidden_width = gate_ref.shape[1]
    router = jnp.broadcast_to(router_ref[...], (hidden_width, members.shape[1]))
    parts = (
        jnp.dot(members, gate_ref[...], preferred_element_type=jnp.float32),
        jnp.dot(members, up_ref[...], preferred_element_type=jnp.float32),
        lax.dot_general(
            members, router, (((1,), (1,)), ((), ())), preferred_element_type=jnp.float32
        ),
    )
    for k, part in enumerate(parts):
        own_ref[:, k * hidden_width : (k + 1) * hidden_width] = part
        sent_ref[:, k * hidden_width : (k + 1) * hidden_width] = part.astype(jnp.bfloat16)


def expert_out_kernel(own_ref, other_ref, down_ref, out_ref):
    both = own_ref[...] + other_ref[...].astype(jnp.float32)
    hidden_width = down_ref.shape[0]
    gate = both[:, :hidden_width]
    up = both[:, hidden_width : 2 * hidden_width]
    score = both[:, 2 * hidden_width :]
    weight = 1.0 / (1.0 + jnp.exp(-score))
    gated = weight * gate
    hidden = (gated / (1.0 + jnp.exp(-gated)) * (weight * up)).astype(jnp.bfloat16)
    out_ref[...] = jnp.dot(hidden, down_ref[...], preferred_element_type=jnp.float32).astype(
        jnp.bfloat16
    )


def summed(*parts):
    total = parts[0].astype(jnp.float32)
    for part in parts[1:]:
        total = total + part.astype(jnp.float32)
    return total.astype(jnp.bfloat16)


def shards(queries, keys, values, expert_ids, router, w_gate, w_up, w_down):
    row_count, features = queries.shape[1:]
    ep_count = lax.axis_size("ep")
    far_count = lax.axis_size("far")
    near_count = lax.axis_size("near")
    ctx_count = far_count * near_count
    place = lax.axis_index(CTX)

    def shift(value, step):
        return lax.ppermute(
            value, CTX, [(i, (i + step) % ctx_count) for i in range(ctx_count)]
        )

    chosen = expert_ids[0, :, 0]
    choose = (chosen[:, None] == jnp.arange(ep_count, dtype=jnp.int32)[None, :]).astype(jnp.int32)
    earlier = jnp.cumsum(choose, axis=0) - choose
    slot_index = jnp.sum(earlier * choose, axis=1)
    target = chosen * CAP + slot_index
    spread = (target[None, :] == jnp.arange(ep_count * CAP, dtype=jnp.int32)[:, None]).astype(
        jnp.bfloat16
    )
    hidden_width = w_gate.shape[2]
    kv_heads = keys.shape[2] // HEAD_WIDTH

    q = queries[0]
    own_kv = jnp.concatenate([keys[0], values[0]], axis=1)
    keys_values = lax.all_gather(own_kv, CTX, axis=0, tiled=True)
    key_count = keys_values.shape[0]
    own_chunk = min(OWN_CHUNK, key_count)

    routed_q = jnp.dot(spread, q, preferred_element_type=jnp.float32).astype(jnp.bfloat16)
    routed_row = jnp.sum(
        spread.astype(jnp.float32) * jnp.arange(row_count, dtype=jnp.float32)[None, :],
        axis=1,
        keepdims=True,
    )
    sent_q = jnp.concatenate(
        [routed_q, jnp.broadcast_to(routed_row, (ep_count * CAP, HEAD_WIDTH)).astype(jnp.bfloat16)],
        axis=1,
    )
    far_q = lax.all_gather(sent_q, "far", axis=0)
    far_q = far_q.reshape(far_count, ep_count, CAP, features + HEAD_WIDTH)
    far_q = jnp.transpose(far_q, (1, 0, 2, 3)).reshape(-1, features + HEAD_WIDTH)
    begins = (
        jnp.arange(far_count, dtype=jnp.int32) * near_count + lax.axis_index("near")
    ) * row_count
    set_attended = attend_routed(begins, far_q, keys_values)
    arrived = lax.all_to_all(
        set_attended.reshape(ep_count, far_count * CAP, features), "ep", 0, 0, tiled=True
    )
    own_set = arrived.reshape(ep_count * far_count * CAP, features)

    first_chunk = place * row_count // own_chunk
    own_span = jnp.stack([first_chunk, place * row_count]).astype(jnp.int32)

    ahead_count = near_count // 2
    back_count = near_count - 1 - ahead_count
    ahead = back = own_set
    ahead_pieces, back_pieces = [], []
    for step in range(1, ahead_count + 1):
        ahead = shift(ahead, 1)
        ahead_pieces.append(ahead)
        if step <= back_count:
            back = shift(back, -1)
            back_pieces.append(back)
    pieces = [own_set] + ahead_pieces + back_pieces
    set_rows = own_set.shape[0]
    member_rows = set_rows * near_count

    own_part, sent_part = pl.pallas_call(
        functools.partial(expert_in_kernel, piece_count=near_count),
        out_shape=[
            jax.ShapeDtypeStruct((member_rows, 3 * hidden_width), jnp.float32),
            jax.ShapeDtypeStruct((member_rows, 3 * hidden_width), jnp.bfloat16),
        ],
        compiler_params=pltpu.CompilerParams(vmem_limit_bytes=24 * 1024 * 1024),
        name="expert_in",
        interpret=INTERPRET,
    )(*pieces, w_gate[0], w_up[0], router.reshape(1, features))
    other_part = lax.ppermute(sent_part, "tp", [(0, 1), (1, 0)])
    partial_out = pl.pallas_call(
        expert_out_kernel,
        out_shape=jax.ShapeDtypeStruct((member_rows, features), jnp.bfloat16),
        compiler_params=pltpu.CompilerParams(vmem_limit_bytes=24 * 1024 * 1024),
        name="expert_out",
        interpret=INTERPRET,
    )(own_part, other_part, w_down[0])
    parts = [partial_out[k * set_rows : (k + 1) * set_rows] for k in range(near_count)]
    own_out = parts[0]
    ahead_out = parts[1 : 1 + ahead_count]
    back_out = parts[1 + ahead_count :]
    ahead_sum, back_sum = ahead_out[-1], back_out[-1]
    for step in range(ahead_count - 1, -1, -1):
        ahead_sum = shift(ahead_sum, -1)
        if step:
            ahead_sum = summed(ahead_out[step - 1], ahead_sum)
    for step in range(back_count - 1, -1, -1):
        back_sum = shift(back_sum, 1)
        if step:
            back_sum = summed(back_out[step - 1], back_sum)
    set_sum = summed(own_out, ahead_sum, back_sum)
    set_sum, own_q = lax.optimization_barrier((set_sum, q))
    attended = attend(own_span, own_q, keys_values, 0, kv_heads, own_chunk)
    returned = lax.all_to_all(
        set_sum.reshape(ep_count * far_count, CAP, features), ("ep", "far"), 0, 0, tiled=True
    )
    expert_rows = jnp.sum(
        returned.reshape(ep_count, far_count, CAP, features).astype(jnp.float32), axis=1
    ).astype(jnp.bfloat16).reshape(ep_count * CAP, features)
    routed = lax.dot_general(
        spread, expert_rows, (((0,), (0,)), ((), ())), preferred_element_type=jnp.float32
    )
    layer_out = (attended.astype(jnp.float32) + routed).astype(jnp.bfloat16)
    return layer_out[None]


def solution(mesh):
    shape = dict(zip(mesh.axis_names, mesh.devices.shape))
    near = NEAR if shape["ctx"] % NEAR == 0 else shape["ctx"]
    names, sizes = [], []
    for name in mesh.axis_names:
        if name == "ctx":
            names += ["far", "near"]
            sizes += [shape[name] // near, near]
        else:
            names.append(name)
            sizes.append(shape[name])
    split = Mesh(mesh.devices.reshape(sizes), tuple(names))
    placed = (
        P(("groups", "ep"), CTX, "tp"),
        P(("groups", "ep"), CTX, "tp"),
        P(("groups", "ep"), CTX, "tp"),
        P(("groups", "ep"), CTX, None),
        P("tp", "ep"),
        P("ep", "tp", CTX),
        P("ep", "tp", CTX),
        P("ep", CTX, "tp"),
    )
    return jax.shard_map(
        shards,
        mesh=split,
        in_specs=placed,
        out_specs=P(("groups", "ep"), CTX, "tp"),
        check_vma=False,
    )
```
